32 devices in a mesh: gr: 8 (over z, core), gc: 4 (over y, x).
Axes of the slice: x: 2, y: 2, z: 4, core: 2. Of those that a mesh axis runs over, the one named last changes fastest.
Arguments:
- projectors: bfloat16 [2, 8192, 9216], P(None, ('gr', 'gc')), may hold values from -0.0625 to 0.0625
- wavefunctions: bfloat16 [2, 8192, 512], P(None, ('gr', 'gc')), may hold values from -6 to 6
- coupling: float32 [512, 18, 18], P('gc'), may hold values from -1.5 to 1.5
- atom_order: int32 [512], replicated, may hold values from 0 to 511, each once
Outputs:
- coupled: float32 [9216, 512], P('gc', 'gr')
The draws below stay inside these ranges and needn't reach their ends.
Inputs may be any that keep to these rules, and one draw needn't show every extreme that they name: `atom_order`: a permutation of the atoms.
All inputs are finite; a program needn't handle non-finite values.
Results may differ from the reference program's by a relative error of at most 0.0003.
Values sent between devices are 32-bit elements; how exact they have to be, the bound alone decides.
A program may use at most 128 MiB of HBM per device.

```python
import jax
import jax.numpy as jnp
from jax import lax

ATOMS = 512
NH = 18
BANDS = 512
NKB = 9216
NPW = 8192


def spiked(drawn, key, source, target, parts, factor):
    def block_of(position):
        return (jnp.arange(drawn.shape[position]) // (drawn.shape[position] // parts)).reshape((-1,) + (1,) * (drawn.ndim - 1 - position))

    first = jax.random.permutation(key, parts)[block_of(target)]
    second = (block_of(target) + parts // 2) % parts
    return jnp.where((block_of(source) == first) | (block_of(source) == second), factor * drawn, drawn)


def block_scale(own_key, extent, cuts, least, largest):
    level, own = 1.0, jax.random.fold_in(own_key, 6)
    for dim, blocks in cuts:
        heights = jnp.exp(jax.random.uniform(jax.random.fold_in(own, dim), (blocks,), jnp.float32, least / len(cuts), largest / len(cuts)))
        level = level * jnp.repeat(heights, extent[dim] // blocks).reshape([-1 if axis == dim else 1 for axis in range(len(extent))])
    return level


def scatter_about(own_key, shape, width, reach, split=(), dtype=jnp.bfloat16):
    drawn = jax.random.normal(own_key, shape, jnp.float32) * width
    if len(split) > 0:
        drawn = block_scale(own_key, shape, split, -0.22, 0.18) * drawn
    return jnp.clip(drawn, min=-reach, max=reach).astype(dtype)


def heavy_noise(key, extent, width, reach, split, heavy, dtype=jnp.bfloat16):
    drawn = width * jax.random.normal(key, extent, jnp.float32)
    if split:
        drawn = drawn * block_scale(key, extent, split, -0.22, 0.18)
    return jnp.clip(spiked(drawn, jax.random.fold_in(key, 3), *heavy), -reach, reach).astype(dtype)


def setup_inputs(seed: int = 0) -> dict:
    seeds = jax.random.split(jax.random.key(seed), 5)
    return {
        "projectors": heavy_noise(seeds[0], (2, NPW, NKB), (4 * NPW) ** -0.5, 0.0625, ((1, 32),), (1, 2, 32, 2.75)),
        "wavefunctions": scatter_about(seeds[1], (2, NPW, BANDS), 1.0, 6.0, ((1, 32),)),
        "coupling": scatter_about(seeds[2], (ATOMS, NH, NH), NH ** -0.5, 1.5, ((0, 4),), jnp.float32),
        "atom_order": jax.random.permutation(seeds[3], ATOMS).astype(jnp.int32),
    }


def reference(projectors, wavefunctions, coupling, atom_order):
    shaped = projectors.reshape(2, NPW, ATOMS, NH)
    waves = wavefunctions.reshape(2 * NPW, BANDS)
    blocks = atom_order.reshape(-1, 32)

    def one_block(picked_ids):
        columns = jnp.take(shaped, picked_ids, axis=2).reshape(2 * NPW, 32 * NH)
        term = lax.dot_general(columns, waves, (((0,), (0,)), ((), ())), preferred_element_type=jnp.float32)
        return 2.0 * term

    becp = lax.map(one_block, blocks).reshape(ATOMS, NH, BANDS)
    coupled = jnp.einsum("kij,kjb->kib", coupling.astype(jnp.float32), becp, precision=lax.Precision.HIGHEST)
    return coupled.reshape(NKB, BANDS)
```

```python
import functools
import math

import jax
import jax.numpy as jnp
from jax import lax
from jax.experimental import pallas as pl
from jax.experimental.pallas import tpu as pltpu
from jax.sharding import PartitionSpec as P

MESH = pl.DeviceIdType.MESH
GROUP = 4
LANES = 128


def plain(projectors, wavefunctions, coupling, atom_order):
    rows_here, nkb = projectors.shape[1:]
    bands = wavefunctions.shape[2]
    atoms = atom_order.shape[0]
    nh = nkb // atoms
    shaped = projectors.reshape(2, rows_here, atoms, nh)
    waves = wavefunctions.reshape(2 * rows_here, bands)
    columns = jnp.take(shaped, atom_order, axis=2).reshape(2 * rows_here, nkb)
    term = lax.dot_general(columns, waves, (((0,), (0,)), ((), ())), preferred_element_type=jnp.float32)
    partial_rows = lax.psum_scatter(2.0 * term, "gc", scatter_dimension=0, tiled=True)
    becp = lax.psum_scatter(partial_rows, "gr", scatter_dimension=1, tiled=True)
    local_atoms = coupling.shape[0]
    becp = becp.reshape(local_atoms, nh, becp.shape[1])
    coupled = jnp.einsum("kij,kjb->kib", coupling, becp, precision=lax.Precision.HIGHEST)
    return coupled.reshape(local_atoms * nh, becp.shape[2])


def path_of(column):
    first, other = ("A", "B") if column % 2 == 0 else ("B", "A")
    order = (first, other, "Z") if (column // 2) % 3 == 1 else (first, "Z", other)
    return order, (1 if column % 2 == 0 else -1)


def kernel(size, nh, apo, columns, order_ref, term_ref, coup_ref, out_ref, nat, acc, oth, rec, nat_sem, send_sem, recv_sem):
    gr, gc = lax.axis_index("gr"), lax.axis_index("gc")
    core, z = lax.rem(gr, 2), gr // 2
    me = {"A": gc // size["B"], "B": lax.rem(gc, size["B"]), "Z": z}
    half = apo // 2

    loads = [
        pltpu.make_async_copy(term_ref.at[:, pl.ds(i * LANES, LANES)], nat.at[i], nat_sem.at[i])
        for i in range(size["Z"])
    ]
    for load in loads:
        load.start()

    def neighbour(dim, way):
        n = size[dim]
        place = lax.rem(me[dim] + n + way, n)
        if dim == "A":
            return {"gr": gr, "gc": place * size["B"] + me["B"]}
        if dim == "B":
            return {"gr": gr, "gc": me["A"] * size["B"] + place}
        return {"gr": place * 2 + core, "gc": gc}

    partner = {"gr": gr + 1 - 2 * core, "gc": gc}
    greeted = [partner]
    for dim in ("A", "B", "Z"):
        if size[dim] > 1:
            greeted.append(neighbour(dim, 1))
        if size[dim] > 2:
            greeted.append(neighbour(dim, -1))
    barrier = pltpu.get_barrier_semaphore()
    for device in greeted:
        pl.semaphore_signal(barrier, inc=1, device_id=device, device_id_type=MESH)
    pl.semaphore_wait(barrier, len(greeted))

    for load in loads:
        load.wait()

    def copy(src, dst, column, slot, device):
        return pltpu.make_async_remote_copy(
            src_ref=src, dst_ref=dst, send_sem=send_sem.at[column, slot], recv_sem=recv_sem.at[column, slot],
            device_id=device, device_id_type=MESH,
        )

    def pack(dst, which, column):
        path, _ = path_of(column)

        def body(owner, carry):
            at = {"A": owner // size["B"], "B": lax.rem(owner, size["B"])}
            for i in range(GROUP):
                row = order_ref[owner * apo + which * half + column * GROUP + i] * nh
                for zz in range(size["Z"]):
                    at["Z"] = zz
                    where = tuple(at[d] for d in path)
                    dst[where + (pl.ds(i * nh, nh), slice(None))] = nat[zz, pl.ds(row, nh), :]
            return carry

        lax.fori_loop(0, size["A"] * size["B"], body, 0)

    def add(dst, prefix, src, src_prefix, rest):
        def body(t, carry):
            where = []
            for n in reversed(rest):
                where.insert(0, lax.rem(t, n))
                t = t // n
            where = tuple(where)
            dst[tuple(prefix) + where] = dst[tuple(prefix) + where] + src[tuple(src_prefix) + where]
            return carry

        if rest:
            lax.fori_loop(0, math.prod(rest), body, 0)
        else:
            dst[tuple(prefix)] = dst[tuple(prefix)] + src[tuple(src_prefix)]

    def steps_of(column):
        path, way = path_of(column)
        found = []
        for stage, dim in enumerate(path):
            n = size[dim]
            turn = way if dim == "Z" else 1
            fixed = [me[d] for d in path[:stage]]
            rest = [size[d] for d in path[stage + 1:]]
            for t in range(n - 1):
                sent = lax.rem(me[dim] - turn * (t + 1) + 2 * n, n)
                got = lax.rem(me[dim] - turn * (t + 2) + 2 * n, n)
                found.append((stage, t, fixed + [sent], fixed + [got], rest, neighbour(dim, turn)))
        return found

    started = {}

    def begin(column, slot, made):
        started[column, slot] = made
        made.start()

    def send_step(column, number):
        stage, t, sent, _, _, device = steps[column][number]
        begin(column, number + 1, copy(acc[column].at[tuple(sent)], rec[column][stage + 1].at[t], column, number + 1, device))

    steps = [steps_of(c) for c in range(columns)]
    n_steps = len(steps[0])

    def phase(number, c):
        if number == 0:
            pack(oth[c], 1 - core, c)
            begin(c, 0, copy(oth[c], rec[c][0], c, 0, partner))
            pack(acc[c], core, c)
            return
        started[c, number - 1].wait_recv()
        if number == 1:
            path, _ = path_of(c)
            add(acc[c], (), rec[c][0], (), [size[d] for d in path])
        else:
            stage, t, _, got, rest, _ = steps[c][number - 2]
            add(acc[c], got, rec[c][stage + 1], [t], rest)
        if number <= n_steps:
            send_step(c, number - 1)
            return
        path, _ = path_of(c)
        mine = tuple(me[d] for d in path)
        for i in range(GROUP):
            becp = 2.0 * acc[c][mine + (pl.ds(i * nh, nh), slice(None))]
            out_ref[core, c, pl.ds(i * nh, nh), :] = jnp.dot(
                coup_ref[core * half + c * GROUP + i], becp,
                precision=lax.Precision.HIGHEST, preferred_element_type=jnp.float32,
            )
        begin(c, n_steps + 1, copy(out_ref.at[core, c], out_ref.at[core, c], c, n_steps + 1, partner))

    lag = [0, 1] + [2 * i + 1 for i in range(1, n_steps + 1)]
    for tick in range(columns + lag[-1]):
        for number in reversed(range(n_steps + 2)):
            c = tick - lag[number]
            if 0 <= c < columns:
                phase(number, c)
    for c in range(columns):
        started[c, n_steps + 1].wait_recv()
        for slot in range(n_steps + 2):
            started[c, slot].wait_send()


def routed(size, projectors, wavefunctions, coupling, atom_order):
    rows_here, nkb = projectors.shape[1:]
    bands = wavefunctions.shape[2]
    atoms = atom_order.shape[0]
    nh, apo = nkb // atoms, coupling.shape[0]
    columns = apo // 2 // GROUP
    n_steps = sum(size.values()) - 3
    tile = (GROUP * nh, LANES)
    term = lax.dot_general(
        projectors.reshape(2 * rows_here, nkb), wavefunctions.reshape(2 * rows_here, bands),
        (((0,), (0,)), ((), ())), preferred_element_type=jnp.float32,
    )
    acc, rec = [], []
    for c in range(columns):
        n1, n2, n3 = (size[d] for d in path_of(c)[0])
        acc.append(pltpu.VMEM((n1, n2, n3) + tile, jnp.float32))
        rec.append([
            pltpu.VMEM((n1, n2, n3) + tile, jnp.float32),
            pltpu.VMEM((n1 - 1, n2, n3) + tile, jnp.float32),
            pltpu.VMEM((n2 - 1, n3) + tile, jnp.float32),
            pltpu.VMEM((n3 - 1,) + tile, jnp.float32),
        ])
    out = pl.pallas_call(
        functools.partial(kernel, size, nh, apo, columns),
        out_shape=jax.ShapeDtypeStruct((2, columns) + tile, jnp.float32),
        in_specs=[
            pl.BlockSpec(memory_space=pltpu.SMEM),
            pl.BlockSpec(memory_space=pl.ANY),
            pl.BlockSpec(memory_space=pltpu.VMEM),
        ],
        out_specs=pl.BlockSpec(memory_space=pltpu.VMEM),
        scratch_shapes=[
            pltpu.VMEM((size["Z"], nkb, LANES), jnp.float32),
            acc,
            list(acc),
            rec,
            pltpu.SemaphoreType.DMA((size["Z"],)),
            pltpu.SemaphoreType.DMA((columns, n_steps + 2)),
            pltpu.SemaphoreType.DMA((columns, n_steps + 2)),
        ],
        compiler_params=pltpu.CompilerParams(
            collective_id=0, has_side_effects=True, vmem_limit_bytes=67_043_328
        ),
    )(atom_order, term, coupling)
    out = out.reshape(apo * nh, LANES)
    own = LANES // 2
    return jnp.where(lax.rem(lax.axis_index("gr"), 2) == 0, out[:, :own], out[:, own:])


def solution(mesh):
    gr, gc = mesh.shape["gr"], mesh.shape["gc"]
    wide = max(d for d in range(1, math.isqrt(gc) + 1) if gc % d == 0)
    size = {"A": wide, "B": gc // wide, "Z": gr // 2}

    def shards(projectors, wavefunctions, coupling, atom_order):
        fits = (
            gr % 2 == 0
            and min(size.values()) > 1
            and wavefunctions.shape[2] == size["Z"] * LANES
            and coupling.shape[0] % (2 * GROUP) == 0
        )
        if fits:
            return routed(size, projectors, wavefunctions, coupling, atom_order)
        return plain(projectors, wavefunctions, coupling, atom_order)

    return jax.shard_map(
        shards,
        mesh=mesh,
        in_specs=(
            P(None, ("gr", "gc"), None),
            P(None, ("gr", "gc"), None),
            P("gc", None, None),
            P(),
        ),
        out_specs=P("gc", "gr"),
        check_vma=False,
    )
```

```python
import functools
import math

import jax
import jax.numpy as jnp
from jax import lax
from jax.experimental import pallas as pl
from jax.experimental.pallas import tpu as pltpu
from jax.sharding import PartitionSpec as P

MESH = pl.DeviceIdType.MESH
GROUP = 4
LANES = 128
PART = 1152


def plain(projectors, wavefunctions, coupling, atom_order):
    rows_here, nkb = projectors.shape[1:]
    bands = wavefunctions.shape[2]
    atoms = atom_order.shape[0]
    nh = nkb // atoms
    shaped = projectors.reshape(2, rows_here, atoms, nh)
    waves = wavefunctions.reshape(2 * rows_here, bands)
    columns = jnp.take(shaped, atom_order, axis=2).reshape(2 * rows_here, nkb)
    term = lax.dot_general(columns, waves, (((0,), (0,)), ((), ())), preferred_element_type=jnp.float32)
    partial_rows = lax.psum_scatter(2.0 * term, "gc", scatter_dimension=0, tiled=True)
    becp = lax.psum_scatter(partial_rows, "gr", scatter_dimension=1, tiled=True)
    local_atoms = coupling.shape[0]
    becp = becp.reshape(local_atoms, nh, becp.shape[1])
    coupled = jnp.einsum("kij,kjb->kib", coupling, becp, precision=lax.Precision.HIGHEST)
    return coupled.reshape(local_atoms * nh, becp.shape[2])


def path_of(column):
    first, other = ("A", "B") if column % 2 == 0 else ("B", "A")
    order = (first, other, "Z") if (column // 2) % 3 == 1 else (first, "Z", other)
    return order, (1 if column % 2 == 0 else -1)


def divisor(total, most):
    return max(t for t in range(LANES, most + 1, LANES) if total % t == 0)


def kernel(
    size, nh, apo, columns, order_ref, proj_ref, wave_ref, coup_ref, out_ref, nat, strip, acc, oth, rec, strip_sem, send_sem, recv_sem
):
    gr, gc = lax.axis_index("gr"), lax.axis_index("gc")
    core, z = lax.rem(gr, 2), gr // 2
    me = {"A": gc // size["B"], "B": lax.rem(gc, size["B"]), "Z": z}
    half = apo // 2

    slots, _, width = strip.shape
    strips = proj_ref.shape[1] // width

    def load(number):
        slot = number % slots
        return pltpu.make_async_copy(proj_ref.at[:, pl.ds(number * width, width)], strip.at[slot], strip_sem.at[slot])

    for number in range(slots):
        load(number).start()

    def neighbour(dim, way):
        n = size[dim]
        place = lax.rem(me[dim] + n + way, n)
        if dim == "A":
            return {"gr": gr, "gc": place * size["B"] + me["B"]}
        if dim == "B":
            return {"gr": gr, "gc": me["A"] * size["B"] + place}
        return {"gr": place * 2 + core, "gc": gc}

    partner = {"gr": gr + 1 - 2 * core, "gc": gc}
    greeted = [partner]
    for dim in ("A", "B", "Z"):
        if size[dim] > 1:
            greeted.append(neighbour(dim, 1))
        if size[dim] > 2:
            greeted.append(neighbour(dim, -1))
    barrier = pltpu.get_barrier_semaphore()
    for device in greeted:
        pl.semaphore_signal(barrier, inc=1, device_id=device, device_id_type=MESH)

    part = divisor(width, PART)
    for number in range(strips):
        load(number).wait()

        def multiply(t, carry, number=number):
            at = pl.multiple_of(t * part, part)
            term = lax.dot_general(
                strip[number % slots, :, pl.ds(at, part)], wave_ref[...],
                (((0,), (0,)), ((), ())), preferred_element_type=jnp.float32,
            )
            for zz in range(size["Z"]):
                nat[zz, pl.ds(number * width + at, part), :] = term[:, zz * LANES:(zz + 1) * LANES]
            return carry

        lax.fori_loop(0, width // part, multiply, 0)
        if number + slots < strips:
            load(number + slots).start()
    pl.semaphore_wait(barrier, len(greeted))

    def copy(src, dst, column, slot, device):
        return pltpu.make_async_remote_copy(
            src_ref=src, dst_ref=dst, send_sem=send_sem.at[column, slot], recv_sem=recv_sem.at[column, slot],
            device_id=device, device_id_type=MESH,
        )

    def pack(dst, which, column):
        path, _ = path_of(column)

        def body(owner, carry):
            at = {"A": owner // size["B"], "B": lax.rem(owner, size["B"])}
            for i in range(GROUP):
                row = order_ref[owner * apo + which * half + column * GROUP + i] * nh
                for zz in range(size["Z"]):
                    at["Z"] = zz
                    where = tuple(at[d] for d in path)
                    dst[where + (pl.ds(i * nh, nh), slice(None))] = nat[zz, pl.ds(row, nh), :]
            return carry

        lax.fori_loop(0, size["A"] * size["B"], body, 0)

    def add(dst, prefix, src, src_prefix, rest):
        def body(t, carry):
            where = []
            for n in reversed(rest):
                where.insert(0, lax.rem(t, n))
                t = t // n
            where = tuple(where)
            dst[tuple(prefix) + where] = dst[tuple(prefix) + where] + src[tuple(src_prefix) + where]
            return carry

        if rest:
            lax.fori_loop(0, math.prod(rest), body, 0)
        else:
            dst[tuple(prefix)] = dst[tuple(prefix)] + src[tuple(src_prefix)]

    def steps_of(column):
        path, way = path_of(column)
        found = []
        for stage, dim in enumerate(path):
            n = size[dim]
            turn = way if dim == "Z" else 1
            fixed = [me[d] for d in path[:stage]]
            rest = [size[d] for d in path[stage + 1:]]
            for t in range(n - 1):
                sent = lax.rem(me[dim] - turn * (t + 1) + 2 * n, n)
                got = lax.rem(me[dim] - turn * (t + 2) + 2 * n, n)
                found.append((stage, t, fixed + [sent], fixed + [got], rest, neighbour(dim, turn)))
        return found

    started = {}

    def begin(column, slot, made):
        started[column, slot] = made
        made.start()

    def send_step(column, number):
        stage, t, sent, _, _, device = steps[column][number]
        begin(column, number + 1, copy(acc[column].at[tuple(sent)], rec[column][stage + 1].at[t], column, number + 1, device))

    steps = [steps_of(c) for c in range(columns)]
    n_steps = len(steps[0])

    def phase(number, c):
        if number == 0:
            pack(oth[c], 1 - core, c)
            begin(c, 0, copy(oth[c], rec[c][0], c, 0, partner))
            pack(acc[c], core, c)
            return
        started[c, number - 1].wait_recv()
        if number == 1:
            path, _ = path_of(c)
            add(acc[c], (), rec[c][0], (), [size[d] for d in path])
        else:
            stage, t, _, got, rest, _ = steps[c][number - 2]
            add(acc[c], got, rec[c][stage + 1], [t], rest)
        if number <= n_steps:
            send_step(c, number - 1)
            return
        path, _ = path_of(c)
        mine = tuple(me[d] for d in path)
        for i in range(GROUP):
            becp = 2.0 * acc[c][mine + (pl.ds(i * nh, nh), slice(None))]
            out_ref[core, c, pl.ds(i * nh, nh), :] = jnp.dot(
                coup_ref[core * half + c * GROUP + i], becp,
                precision=lax.Precision.HIGHEST, preferred_element_type=jnp.float32,
            )
        begin(c, n_steps + 1, copy(out_ref.at[core, c], out_ref.at[core, c], c, n_steps + 1, partner))

    lag = [0, 1] + [3 * i + 1 for i in range(1, n_steps + 1)]
    for tick in range(columns + lag[-1]):
        for number in reversed(range(n_steps + 2)):
            c = tick - lag[number]
            if 0 <= c < columns:
                phase(number, c)
    for c in range(columns):
        started[c, n_steps + 1].wait_recv()
        for slot in range(n_steps + 2):
            started[c, slot].wait_send()


def routed(size, projectors, wavefunctions, coupling, atom_order):
    rows_here, nkb = projectors.shape[1:]
    bands = wavefunctions.shape[2]
    atoms = atom_order.shape[0]
    nh, apo = nkb // atoms, coupling.shape[0]
    columns = apo // 2 // GROUP
    n_steps = sum(size.values()) - 3
    tile = (GROUP * nh, LANES)
    width = divisor(nkb, 1152)
    acc, rec = [], []
    for c in range(columns):
        n1, n2, n3 = (size[d] for d in path_of(c)[0])
        acc.append(pltpu.VMEM((n1, n2, n3) + tile, jnp.float32))
        rec.append([
            pltpu.VMEM((n1, n2, n3) + tile, jnp.float32),
            pltpu.VMEM((n1 - 1, n2, n3) + tile, jnp.float32),
            pltpu.VMEM((n2 - 1, n3) + tile, jnp.float32),
            pltpu.VMEM((n3 - 1,) + tile, jnp.float32),
        ])
    out = pl.pallas_call(
        functools.partial(kernel, size, nh, apo, columns),
        out_shape=jax.ShapeDtypeStruct((2, columns) + tile, jnp.float32),
        in_specs=[
            pl.BlockSpec(memory_space=pltpu.SMEM),
            pl.BlockSpec(memory_space=pl.ANY),
            pl.BlockSpec(memory_space=pltpu.VMEM),
            pl.BlockSpec(memory_space=pltpu.VMEM),
        ],
        out_specs=pl.BlockSpec(memory_space=pltpu.VMEM),
        scratch_shapes=[
            pltpu.VMEM((size["Z"], nkb, LANES), jnp.float32),
            pltpu.VMEM((3, 2 * rows_here, width), projectors.dtype),
            acc,
            list(acc),
            rec,
            pltpu.SemaphoreType.DMA((3,)),
            pltpu.SemaphoreType.DMA((columns, n_steps + 2)),
            pltpu.SemaphoreType.DMA((columns, n_steps + 2)),
        ],
        compiler_params=pltpu.CompilerParams(
            collective_id=0, has_side_effects=True, vmem_limit_bytes=67_043_328
        ),
    )(
        atom_order, projectors.reshape(2 * rows_here, nkb), wavefunctions.reshape(2 * rows_here, bands), coupling
    )
    out = out.reshape(apo * nh, LANES)
    own = LANES // 2
    return jnp.where(lax.rem(lax.axis_index("gr"), 2) == 0, out[:, :own], out[:, own:])


def solution(mesh):
    gr, gc = mesh.shape["gr"], mesh.shape["gc"]
    wide = max(d for d in range(1, math.isqrt(gc) + 1) if gc % d == 0)
    size = {"A": wide, "B": gc // wide, "Z": gr // 2}

    def shards(projectors, wavefunctions, coupling, atom_order):
        fits = (
            gr % 2 == 0
            and min(size.values()) > 1
            and wavefunctions.shape[2] == size["Z"] * LANES
            and coupling.shape[0] % (2 * GROUP) == 0
        )
        if fits:
            return routed(size, projectors, wavefunctions, coupling, atom_order)
        return plain(projectors, wavefunctions, coupling, atom_order)

    return jax.shard_map(
        shards,
        mesh=mesh,
        in_specs=(
            P(None, ("gr", "gc"), None),
            P(None, ("gr", "gc"), None),
            P("gc", None, None),
            P(),
        ),
        out_specs=P("gc", "gr"),
        check_vma=False,
    )
```

```python
import functools
import math

import jax
import jax.numpy as jnp
from jax import lax
from jax.experimental import pallas as pl
from jax.experimental.pallas import tpu as pltpu
from jax.sharding import PartitionSpec as P

MESH = pl.DeviceIdType.MESH
GROUP = 4
LANES = 128
PART = 1152


def plain(projectors, wavefunctions, coupling, atom_order):
    rows_here, nkb = projectors.shape[1:]
    bands = wavefunctions.shape[2]
    atoms = atom_order.shape[0]
    nh = nkb // atoms
    shaped = projectors.reshape(2, rows_here, atoms, nh)
    waves = wavefunctions.reshape(2 * rows_here, bands)
    columns = jnp.take(shaped, atom_order, axis=2).reshape(2 * rows_here, nkb)
    term = lax.dot_general(columns, waves, (((0,), (0,)), ((), ())), preferred_element_type=jnp.float32)
    partial_rows = lax.psum_scatter(2.0 * term, "gc", scatter_dimension=0, tiled=True)
    becp = lax.psum_scatter(partial_rows, "gr", scatter_dimension=1, tiled=True)
    local_atoms = coupling.shape[0]
    becp = becp.reshape(local_atoms, nh, becp.shape[1])
    coupled = jnp.einsum("kij,kjb->kib", coupling, becp, precision=lax.Precision.HIGHEST)
    return coupled.reshape(local_atoms * nh, becp.shape[2])


def path_of(column):
    first, other = ("A", "B") if column % 2 == 0 else ("B", "A")
    order = (first, other, "Z") if (column // 2) % 3 == 1 else (first, "Z", other)
    return order, (1 if column % 2 == 0 else -1)


def divisor(total, most):
    return max(t for t in range(LANES, most + 1, LANES) if total % t == 0)


def kernel(
    size, nh, apo, columns, order_ref, proj_ref, wave_ref, coup_ref, out_ref, fin, mats, nat, strip, acc, oth, rec, strip_sem, send_sem, recv_sem
):
    gr, gc = lax.axis_index("gr"), lax.axis_index("gc")
    core, z = lax.rem(gr, 2), gr // 2
    me = {"A": gc // size["B"], "B": lax.rem(gc, size["B"]), "Z": z}
    half = apo // 2

    slots, _, width = strip.shape
    strips = proj_ref.shape[1] // width

    def load(number):
        slot = number % slots
        return pltpu.make_async_copy(proj_ref.at[:, pl.ds(number * width, width)], strip.at[slot], strip_sem.at[slot])

    for number in range(slots):
        load(number).start()

    def neighbour(dim, way):
        n = size[dim]
        place = lax.rem(me[dim] + n + way, n)
        if dim == "A":
            return {"gr": gr, "gc": place * size["B"] + me["B"]}
        if dim == "B":
            return {"gr": gr, "gc": me["A"] * size["B"] + place}
        return {"gr": place * 2 + core, "gc": gc}

    partner = {"gr": gr + 1 - 2 * core, "gc": gc}
    greeted = [partner]
    for dim in ("A", "B", "Z"):
        if size[dim] > 1:
            greeted.append(neighbour(dim, 1))
        if size[dim] > 2:
            greeted.append(neighbour(dim, -1))
    barrier = pltpu.get_barrier_semaphore()
    for device in greeted:
        pl.semaphore_signal(barrier, inc=1, device_id=device, device_id_type=MESH)

    part = divisor(width, PART)
    for number in range(strips):
        load(number).wait()

        def multiply(t, carry, number=number):
            at = pl.multiple_of(t * part, part)
            term = lax.dot_general(
                strip[number % slots, :, pl.ds(at, part)], wave_ref[...],
                (((0,), (0,)), ((), ())), preferred_element_type=jnp.float32,
            )
            for zz in range(size["Z"]):
                nat[zz, pl.ds(number * width + at, part), :] = term[:, zz * LANES:(zz + 1) * LANES]
            return carry

        lax.fori_loop(0, width // part, multiply, 0)
        if number + slots < strips:
            load(number + slots).start()
    pl.semaphore_wait(barrier, len(greeted))

    def copy(src, dst, column, slot, device):
        return pltpu.make_async_remote_copy(
            src_ref=src, dst_ref=dst, send_sem=send_sem.at[column, slot], recv_sem=recv_sem.at[column, slot],
            device_id=device, device_id_type=MESH,
        )

    def pack(dst, which, column):
        path, _ = path_of(column)

        def body(owner, carry):
            at = {"A": owner // size["B"], "B": lax.rem(owner, size["B"])}
            for i in range(GROUP):
                row = order_ref[owner * apo + which * half + column * GROUP + i] * nh
                for zz in range(size["Z"]):
                    at["Z"] = zz
                    where = tuple(at[d] for d in path)
                    dst[where + (pl.ds(i * nh, nh), slice(None))] = nat[zz, pl.ds(row, nh), :]
            return carry

        lax.fori_loop(0, size["A"] * size["B"], body, 0)

    def add(dst, prefix, src, src_prefix, rest):
        def body(t, carry):
            where = []
            for n in reversed(rest):
                where.insert(0, lax.rem(t, n))
                t = t // n
            where = tuple(where)
            dst[tuple(prefix) + where] = dst[tuple(prefix) + where] + src[tuple(src_prefix) + where]
            return carry

        if rest:
            lax.fori_loop(0, math.prod(rest), body, 0)
        else:
            dst[tuple(prefix)] = dst[tuple(prefix)] + src[tuple(src_prefix)]

    def steps_of(column):
        path, way = path_of(column)
        found = []
        for stage, dim in enumerate(path):
            n = size[dim]
            turn = way if dim == "Z" else 1
            fixed = [me[d] for d in path[:stage]]
            rest = [size[d] for d in path[stage + 1:]]
            for t in range(n - 1):
                sent = lax.rem(me[dim] - turn * (t + 1) + 2 * n, n)
                got = lax.rem(me[dim] - turn * (t + 2) + 2 * n, n)
                found.append((stage, t, fixed + [sent], fixed + [got], rest, neighbour(dim, turn)))
        return found

    started = {}

    def begin(column, slot, made):
        started[column, slot] = made
        made.start()

    def send_step(column, number):
        stage, t, sent, _, _, device = steps[column][number]
        begin(column, number + 1, copy(acc[column].at[tuple(sent)], rec[column][stage + 1].at[t], column, number + 1, device))

    steps = [steps_of(c) for c in range(columns)]
    n_steps = len(steps[0])

    def phase(number, c):
        if number == 0:
            pack(oth[c], 1 - core, c)
            begin(c, 0, copy(oth[c], rec[c][0], c, 0, partner))
            pack(acc[c], core, c)
            return
        started[c, number - 1].wait_recv()
        if number == 1:
            path, _ = path_of(c)
            add(acc[c], (), rec[c][0], (), [size[d] for d in path])
        else:
            stage, t, _, got, rest, _ = steps[c][number - 2]
            add(acc[c], got, rec[c][stage + 1], [t], rest)
        if number <= n_steps:
            send_step(c, number - 1)
            return
        path, _ = path_of(c)
        mine = tuple(me[d] for d in path)
        at = pl.ds(c * GROUP * nh, GROUP * nh)
        for i in range(GROUP):
            becp = 2.0 * acc[c][mine + (pl.ds(i * nh, nh), slice(None))]
            fin[core, pl.ds((c * GROUP + i) * nh, nh), :] = jnp.dot(
                mats[:, pl.ds(core * half + c * GROUP + i, 1), :].reshape(nh, nh), becp,
                precision=lax.Precision.HIGHEST, preferred_element_type=jnp.float32,
            )
        begin(c, n_steps + 1, copy(fin.at[core, at], fin.at[core, at], c, n_steps + 1, partner))

    lag = [0, 1] + [3 * i + 1 for i in range(1, n_steps + 1)]
    for tick in range(columns + lag[-1]):
        if tick == lag[2]:
            for i in range(nh):
                mats[i] = coup_ref[i].T
        for number in reversed(range(n_steps + 2)):
            c = tick - lag[number]
            if 0 <= c < columns:
                phase(number, c)

    def turn(which):
        rows = fin.shape[1]

        def body(t, carry):
            block = fin[which, pl.ds(pl.multiple_of(t * LANES, LANES), LANES), :].T
            own = LANES // 2
            at = pl.multiple_of(which * rows + t * LANES, LANES)
            out_ref[:, pl.ds(at, LANES)] = jnp.where(core == 0, block[:own], block[own:])
            return carry

        lax.fori_loop(0, rows // LANES, body, 0)

    turn(core)
    for c in range(columns):
        started[c, n_steps + 1].wait_recv()
    turn(1 - core)
    for c in range(columns):
        for slot in range(n_steps + 2):
            started[c, slot].wait_send()


def routed(size, projectors, wavefunctions, coupling, atom_order):
    rows_here, nkb = projectors.shape[1:]
    bands = wavefunctions.shape[2]
    atoms = atom_order.shape[0]
    nh, apo = nkb // atoms, coupling.shape[0]
    columns = apo // 2 // GROUP
    n_steps = sum(size.values()) - 3
    tile = (GROUP * nh, LANES)
    width = divisor(nkb, 1152)
    acc, rec = [], []
    for c in range(columns):
        n1, n2, n3 = (size[d] for d in path_of(c)[0])
        acc.append(pltpu.VMEM((n1, n2, n3) + tile, jnp.float32))
        rec.append([
            pltpu.VMEM((n1, n2, n3) + tile, jnp.float32),
            pltpu.VMEM((n1 - 1, n2, n3) + tile, jnp.float32),
            pltpu.VMEM((n2 - 1, n3) + tile, jnp.float32),
            pltpu.VMEM((n3 - 1,) + tile, jnp.float32),
        ])
    out = pl.pallas_call(
        functools.partial(kernel, size, nh, apo, columns),
        out_shape=jax.ShapeDtypeStruct((LANES // 2, apo * nh), jnp.float32),
        in_specs=[
            pl.BlockSpec(memory_space=pltpu.SMEM),
            pl.BlockSpec(memory_space=pl.ANY),
            pl.BlockSpec(memory_space=pltpu.VMEM),
            pl.BlockSpec(memory_space=pltpu.VMEM),
        ],
        out_specs=pl.BlockSpec(memory_space=pltpu.VMEM),
        scratch_shapes=[
            pltpu.VMEM((2, apo * nh // 2, LANES), jnp.float32),
            pltpu.VMEM((nh, apo, nh), jnp.float32),
            pltpu.VMEM((size["Z"], nkb, LANES), jnp.float32),
            pltpu.VMEM((3, 2 * rows_here, width), projectors.dtype),
            acc,
            list(acc),
            rec,
            pltpu.SemaphoreType.DMA((3,)),
            pltpu.SemaphoreType.DMA((columns, n_steps + 2)),
            pltpu.SemaphoreType.DMA((columns, n_steps + 2)),
        ],
        compiler_params=pltpu.CompilerParams(
            collective_id=0, has_side_effects=True, vmem_limit_bytes=67_043_328
        ),
    )(
        atom_order, projectors.reshape(2 * rows_here, nkb), wavefunctions.reshape(2 * rows_here, bands),
        jnp.transpose(coupling, (1, 2, 0)),
    )
    return out.T


def solution(mesh):
    gr, gc = mesh.shape["gr"], mesh.shape["gc"]
    wide = max(d for d in range(1, math.isqrt(gc) + 1) if gc % d == 0)
    size = {"A": wide, "B": gc // wide, "Z": gr // 2}

    def shards(projectors, wavefunctions, coupling, atom_order):
        fits = (
            gr % 2 == 0
            and min(size.values()) > 1
            and wavefunctions.shape[2] == size["Z"] * LANES
            and coupling.shape[0] % (2 * GROUP) == 0
            and projectors.shape[2] % (2 * gc * LANES) == 0
        )
        if fits:
            return routed(size, projectors, wavefunctions, coupling, atom_order)
        return plain(projectors, wavefunctions, coupling, atom_order)

    return jax.shard_map(
        shards,
        mesh=mesh,
        in_specs=(
            P(None, ("gr", "gc"), None),
            P(None, ("gr", "gc"), None),
            P("gc", None, None),
            P(),
        ),
        out_specs=P("gc", "gr"),
        check_vma=False,
    )
```
